512 devices in a mesh: seq: 128 (over z, y, core), head: 4 (over x).
Axes of the slice: x: 4, y: 8, z: 8, core: 2. Of those that a mesh axis runs over, the one named last changes fastest.
Arguments:
- q_nope: bfloat16 [4, 64, 128], P(None, 'head'), may hold values from -5 to 5
- q_rope: bfloat16 [4, 64, 64], P(None, 'head'), may hold values from -16 to 16
- w_key_up: bfloat16 [64, 128, 512], P('head'), may hold values from -0.5 to 0.5
- w_value_up: bfloat16 [64, 512, 128], P('head'), may hold values from -0.25 to 0.25
- latent_cache: bfloat16 [8192, 64, 576], P('seq'), may hold values from -34 to 34
- page_scale: float32 [8192], P('seq'), may hold values from 0.25 to 2, as said below
- block_table: int32 [4, 2048], P(None, 'seq'), may hold values from 0 to 63, as said below
- lengths: int32 [4], replicated, may hold values from 1 to 131072, 327680 in all
Outputs:
- attn_out: bfloat16 [4, 8192], P('head', 'seq')
The draws below stay inside these ranges and needn't reach their ends.
Inputs may be any that keep to these rules, and one draw needn't show every extreme that they name: `block_table`: each entry is the number of a page within its pool; for each index of seq, the entries of its 16 page columns over all requests name every page of its pool exactly once. `page_scale`: every page scale is positive. `lengths`: each request has at least one cached position and at most 131072; the longest has exactly 131072.
All inputs are finite; a program needn't handle non-finite values.
Results may differ from the reference program's by a relative error of at most 0.0095.
Values may be sent and summed in bfloat16 or wider, within the bound.
A program may use at most 64 MiB of HBM per device.

```python
import math
import jax
import jax.numpy as jnp
import numpy as np
from jax import lax

LAT = 512
ROPE = 64
NOPE = 128
VDIM = 128
HEADS = 64
PAGE = 64
BATCH = 4
BLOCKS_DEV = 16
PAGES_DEV = 64
CTX = 131072
BLOCKS = 2048
PAGES = 8192


def page_scales(key):
    base = jax.random.fold_in(key, 11)
    uniform_draw = jax.random.uniform(base, (PAGES,), jnp.float32)
    scales = jnp.exp(jnp.log(0.5) + uniform_draw * jnp.log(2.0))
    return scales


def rope_signs(key):
    picker = jax.random.uniform(jax.random.fold_in(key, 37), (ROPE,), jnp.float32)
    return jnp.where(picker < 0.5, -1.0, 1.0).astype(jnp.float32)


def draw_page_scale(key, part):
    return page_scales(key).astype(jnp.float32)


def draw_block_table(key, part):
    groups = BLOCKS // BLOCKS_DEV
    subkeys = jax.random.split(key, groups)
    orders = jax.vmap(lambda single: jax.random.permutation(single, PAGES_DEV))(subkeys)
    mapping = orders.reshape(groups, BATCH, BLOCKS_DEV).transpose(1, 0, 2).reshape(BATCH, BLOCKS)
    return mapping.astype(jnp.int32)


def draw_q_rope(key, part):
    base = jax.random.fold_in(key, 41)
    plain = jnp.clip(jax.random.normal(base, (BATCH, HEADS, ROPE), jnp.float32), -5.0, 5.0)
    jitter = jnp.clip(jax.random.normal(jax.random.fold_in(base, 1), (HEADS, ROPE), jnp.float32), -1.0, 1.0)
    aligned = 15.0 * rope_signs(key)[None, :] + jitter
    first_row = (jnp.arange(BATCH, dtype=jnp.int32) == 0)[:, None, None]
    return jnp.where(first_row, aligned[None, :, :], plain).astype(jnp.bfloat16)


def draw_latent_cache(key, part):
    width = LAT + ROPE
    base = jax.random.fold_in(key, 23)
    amp_key, dir_key, noise_key = jax.random.split(base, 3)
    amp_draw = jax.random.uniform(amp_key, (PAGES, 1, 1), jnp.float32)
    amplitude = jnp.exp(jnp.log(0.25) + amp_draw * jnp.log(6.0))
    scales = page_scales(key)
    direction = jnp.clip(jax.random.normal(dir_key, (PAGES, 1, width), jnp.float32), -4.0, 4.0)
    noise = jnp.clip(jax.random.normal(noise_key, (PAGES, PAGE, width), jnp.float32), -4.0, 4.0)
    stored = amplitude * direction + noise
    table = draw_block_table(key, part)
    first_ids = jnp.arange(BLOCKS, dtype=jnp.int32) // BLOCKS_DEV * PAGES_DEV + table[0]
    marked = jnp.zeros((PAGES,), jnp.float32).at[first_ids].set(1.0)
    rope_key = 7.0 * rope_signs(key)[None, None, :] / scales[:, None, None] + noise[:, :, LAT:]
    rope_part = jnp.where(marked[:, None, None] > 0.5, rope_key, stored[:, :, LAT:])
    stored = jnp.concatenate([stored[:, :, :LAT], rope_part], axis=2)
    return stored.astype(jnp.bfloat16)


def level_of(stream_key, extent, pieces, least, largest):
    gain, own = 1.0, jax.random.fold_in(stream_key, 6)
    for position, parts in pieces:
        draws = jnp.exp(jax.random.uniform(jax.random.fold_in(own, position), (parts,), jnp.float32, least / len(pieces), largest / len(pieces)))
        gain = gain * jnp.repeat(draws, extent[position] // parts).reshape([-1 if axis == position else 1 for axis in range(len(extent))])
    return gain


def split_up(amount, total, limit, skew):
    loads = [(1 << 20) // math.isqrt(rank ** skew) + 1 for rank in range(2, amount + 1)]
    surplus, given = total - limit - (amount - 1), [1] * (amount - 1)
    while surplus > 0:
        candidates = [i for i in range(amount - 1) if given[i] < limit]
        pool, left = sum([loads[i] for i in candidates]), surplus
        for i in candidates:
            addition = min(limit - given[i], max(1, left * loads[i] // pool), surplus)
            given[i] = given[i] + addition
            surplus = surplus - addition
    return np.array([limit] + given)


def uneven_parts(stream_key, count, total, reach, slope):
    if count == 2:
        one = jax.random.randint(stream_key, (), max(1, total - reach), min(reach, total - 1) + 1)
        return jnp.stack([one, total - one])
    sizes = jnp.asarray(split_up(count, total, reach, slope), jnp.int32)
    couples = (count - 1) // 2
    source_of, sink = sizes[1:1 + 2 * couples:2], sizes[2:2 + 2 * couples:2]
    margin = jnp.minimum(source_of - 1, reach - sink)
    moved = jax.random.randint(jax.random.fold_in(stream_key, 1), (couples,), 0, 1 << 20) % (margin + 1)
    sizes = sizes.at[1:1 + 2 * couples:2].set(source_of - moved).at[2:2 + 2 * couples:2].set(sink + moved)
    return sizes[jax.random.permutation(jax.random.fold_in(stream_key, 2), count)]


def gaussian(rng, dims, scale, bound, shards=(), kind=jnp.bfloat16):
    values = jax.random.normal(rng, dims, jnp.float32) * scale
    if len(shards) > 0:
        values = level_of(rng, dims, shards, -0.22, 0.18) * values
    return jnp.clip(values, min=-bound, max=bound).astype(kind)


def setup_inputs(seed: int = 0) -> dict:
    seeds = jax.random.split(jax.random.key(seed), 9)
    return {
        "q_nope": gaussian(seeds[0], (BATCH, HEADS, NOPE), 1.0, 5.0, ((1, 4),)),
        "q_rope": draw_q_rope(jax.random.fold_in(seeds[8], 71), 0),
        "w_key_up": gaussian(seeds[2], (HEADS, NOPE, LAT), NOPE ** -0.5, 0.5, ((0, 4),)),
        "w_value_up": gaussian(seeds[3], (HEADS, LAT, VDIM), LAT ** -0.5, 0.25, ((0, 4),)),
        "latent_cache": draw_latent_cache(jax.random.fold_in(seeds[8], 71), 0),
        "page_scale": draw_page_scale(jax.random.fold_in(seeds[8], 71), 0),
        "block_table": draw_block_table(jax.random.fold_in(seeds[8], 71), 0),
        "lengths": uneven_parts(seeds[7], BATCH, 5 * BATCH * CTX // 8, CTX, 0).astype(jnp.int32),
    }


floor_score = -1e30


def reference(q_nope, q_rope, w_key_up, w_value_up, latent_cache, page_scale, block_table, lengths):
    softmax_scale = (NOPE + ROPE) ** -0.5
    q_latent = jnp.einsum("bhn,hnl->bhl", q_nope.astype(jnp.float32), w_key_up.astype(jnp.float32)).astype(jnp.bfloat16)

    def attend(request):
        page_ids = (jnp.arange(BLOCKS, dtype=jnp.int32) // BLOCKS_DEV) * PAGES_DEV + block_table[request]
        cache_rows = latent_cache[page_ids].reshape(CTX, LAT + ROPE)
        scale_rows = jnp.repeat(page_scale[page_ids], PAGE)
        raw_scores = jnp.dot(q_latent[request], cache_rows[:, :LAT].T, preferred_element_type=jnp.float32)
        raw_scores = raw_scores + jnp.dot(q_rope[request], cache_rows[:, LAT:].T, preferred_element_type=jnp.float32)
        usable = jnp.arange(CTX, dtype=jnp.int32) < lengths[request]
        scores = jnp.where(usable[None, :], raw_scores * (scale_rows * softmax_scale)[None, :], floor_score)
        maximum = jnp.max(scores, axis=1, keepdims=True)
        weights = jnp.where(usable[None, :], jnp.exp(scores - maximum), 0.0)
        denominator = jnp.sum(weights, axis=1)
        probabilities = (weights * scale_rows[None, :]).astype(jnp.bfloat16)
        weighted = jnp.dot(probabilities, cache_rows[:, :LAT], preferred_element_type=jnp.float32)
        return weighted / denominator[:, None]

    latent_out = lax.map(attend, jnp.arange(BATCH, dtype=jnp.int32))
    projected = jnp.einsum("bhl,hlv->bhv", latent_out, w_value_up.astype(jnp.float32), precision=lax.Precision.HIGHEST)
    return projected.reshape(BATCH, HEADS * VDIM).astype(jnp.bfloat16)
```

```python
import jax
import jax.numpy as jnp
from jax import lax
from jax.experimental import pallas as pl
from jax.experimental.pallas import tpu as pltpu
from jax.sharding import Mesh
from jax.sharding import PartitionSpec as P

SEQ = ("seq_0", "seq_1", "seq_2")
F32 = jnp.float32
BF16 = jnp.bfloat16
MESH_ID = pl.DeviceIdType.MESH

BATCH = 4
HEADS = 16
ROWS = BATCH * HEADS
LAT = 512
ROPE = 64
NOPE = 128
VDIM = 128
PAGE = 64
PAGES = 64
BLOCKS = 16
CHUNK = 8
CHUNKS = PAGES // CHUNK
SPAN = CHUNK * PAGE
GROUP = 16
NZ = 8
FLOOR = -1e30


def to_column(row, eye):
    return jnp.sum(jnp.where(eye, jnp.broadcast_to(row, eye.shape), 0.0), axis=1, keepdims=True)


def kernel(
    qn_hbm, qr_hbm, wk_hbm, wv_hbm, cache_hbm, ps_hbm, bt_hbm, len_hbm, out_ref,
    qn, qr, wk, wv, cache, ps, bt, ln, qs, qrs, ql, s_buf, vc,
    send_a, recv_a, send_b, recv_b,
    in_sem, cache_sem, a_send, a_recv, b_send, b_recv,
):
    z = lax.axis_index("seq_0")
    y = lax.axis_index("seq_1")
    c = lax.axis_index("seq_2")
    x = lax.axis_index("head")

    small = [
        pltpu.make_async_copy(src, dst, in_sem.at[k])
        for k, (src, dst) in enumerate(
            [(qn_hbm, qn), (qr_hbm, qr), (bt_hbm, bt), (len_hbm, ln), (ps_hbm, ps), (wk_hbm, wk), (wv_hbm, wv)]
        )
    ]
    pages = [
        pltpu.make_async_copy(
            cache_hbm.at[pl.ds(k * CHUNK, CHUNK)], cache.at[pl.ds(k * CHUNK, CHUNK)], cache_sem.at[k]
        )
        for k in range(CHUNKS)
    ]
    for copy in small[:6]:
        copy.start()
    for copy in pages:
        copy.start()
    small[6].start()

    mine = c * 8 + y
    target_z = 2 * x + c
    alone = z == target_z
    barrier = pltpu.get_barrier_semaphore()
    for o in range(1, GROUP):
        peer = lax.rem(mine + o, GROUP)
        pl.semaphore_signal(
            barrier, inc=1, device_id=(z, lax.rem(peer, 8), lax.div(peer, 8), x), device_id_type=MESH_ID
        )
    for k in range(NZ):
        is_self = jnp.logical_and(alone, z == k)

        @pl.when(jnp.logical_not(is_self))
        def _():
            pl.semaphore_signal(
                barrier, inc=1, device_id=(k, y, lax.rem(z, 2), lax.div(z, 2)), device_id_type=MESH_ID
            )

    for copy in small[:5]:
        copy.wait()
    column = lax.broadcasted_iota(jnp.int32, (PAGES, ROWS), 1)
    request = lax.rem(column, BATCH)
    first = ((z * 8 + y) * 2 + c) * (BLOCKS * PAGE)
    page_id = lax.broadcasted_iota(jnp.int32, (PAGES, BLOCKS), 0)
    block = lax.broadcasted_iota(jnp.int32, (PAGES, BLOCKS), 1)
    valid = jnp.zeros((PAGES, ROWS), F32)
    for b in range(BATCH):
        left = jnp.clip(ln[b] - first - block * PAGE, 0, PAGE).astype(F32)
        owned = jnp.where(jnp.broadcast_to(bt[b : b + 1, :], (PAGES, BLOCKS)) == page_id, left, 0.0)
        valid = jnp.where(request == b, jnp.sum(owned, axis=1, keepdims=True), valid)
    vc[...] = valid

    for b in range(BATCH):
        qs[pl.ds(b, HEADS, stride=BATCH), :] = qn[b].astype(F32)
        qrs[pl.ds(b, HEADS, stride=BATCH), :] = qr[b].astype(F32)
    q_rope = qrs[...].astype(BF16)
    small[5].wait()
    for h in range(HEADS):
        lhs = qs[pl.ds(16 * (h // 4), 16), :].astype(BF16)
        part = jnp.dot(lhs, wk[h], preferred_element_type=F32)
        at = 4 * (h % 4)
        ql[pl.ds(4 * h, 4), :] = part[at : at + 4]
    q_lat = ql[...].astype(BF16)

    contract = (((1,), (1,)), ((), ()))
    row_id = lax.broadcasted_iota(jnp.int32, (PAGE, ROWS), 0).astype(F32)
    peak = jnp.full((PAGE, ROWS), FLOOR, F32)
    for k in range(CHUNKS):
        pages[k].wait()
        lat_rows = cache[pl.ds(k * CHUNK, CHUNK), :, :LAT].reshape(SPAN, LAT)
        rope_rows = cache[pl.ds(k * CHUNK, CHUNK), :, LAT:].reshape(SPAN, ROPE)
        raw = lax.dot_general(lat_rows, q_lat, contract, preferred_element_type=F32)
        raw = raw + lax.dot_general(rope_rows, q_rope, contract, preferred_element_type=F32)
        for i in range(CHUNK):
            p = k * CHUNK + i
            scaled = raw[i * PAGE : (i + 1) * PAGE] * (ps[p] * (NOPE + ROPE) ** (-0.5))
            score = jnp.where(row_id < vc[pl.ds(p, 1), :], scaled, FLOOR)
            s_buf[pl.ds(p * PAGE, PAGE), :] = score
            peak = jnp.maximum(peak, score)
    peak = jnp.max(peak, axis=0, keepdims=True)
    floor = jnp.maximum(peak, -1e29)

    total = jnp.zeros((PAGE, ROWS), F32)
    latent = jnp.zeros((ROWS, LAT), F32)
    for k in range(CHUNKS):
        pieces = []
        for i in range(CHUNK):
            p = k * CHUNK + i
            weight = jnp.exp(s_buf[pl.ds(p * PAGE, PAGE), :] - floor)
            total = total + weight
            pieces.append(weight * ps[p])
        prob = jnp.concatenate(pieces, axis=0).T.astype(BF16)
        lat_rows = cache[pl.ds(k * CHUNK, CHUNK), :, :LAT].reshape(SPAN, LAT)
        latent = latent + jnp.dot(prob, lat_rows, preferred_element_type=F32)
    denominator = jnp.sum(total, axis=0, keepdims=True)

    eye = lax.broadcasted_iota(jnp.int32, (ROWS, ROWS), 0) == lax.broadcasted_iota(jnp.int32, (ROWS, ROWS), 1)
    some = denominator > 0.0
    safe = jnp.where(some, denominator, 1.0)
    level = to_column(jnp.where(some, floor + jnp.log(safe), FLOOR), eye)
    inverse = to_column(1.0 / safe, eye)
    level = jnp.broadcast_to(level, (ROWS, VDIM))
    latent = (latent * inverse).astype(BF16)

    small[6].wait()
    for h in range(HEADS):
        part = jnp.dot(latent[16 * (h // 4) : 16 * (h // 4) + 16], wv[h], preferred_element_type=F32)
        at = 4 * (h % 4)
        send_a[h, 0] = part[at : at + 4]
        send_a[h, 1] = level[4 * h : 4 * h + 4]

    pl.semaphore_wait(barrier, GROUP - 1 + NZ - jnp.where(alone, 1, 0))

    first_copies = []
    for o in range(1, GROUP):
        peer = lax.rem(mine + o, GROUP)
        copy = pltpu.make_async_remote_copy(
            src_ref=send_a.at[peer],
            dst_ref=recv_a.at[mine],
            send_sem=a_send.at[o],
            recv_sem=a_recv.at[mine],
            device_id=(z, lax.rem(peer, 8), lax.div(peer, 8), x),
            device_id_type=MESH_ID,
        )
        copy.start()
        first_copies.append(copy)
    recv_a[mine] = send_a[mine]
    for o in range(1, GROUP):
        peer = lax.rem(mine + o, GROUP)
        pltpu.make_async_remote_copy(
            src_ref=send_a.at[peer],
            dst_ref=recv_a.at[peer],
            send_sem=a_send.at[o],
            recv_sem=a_recv.at[peer],
            device_id=(z, lax.rem(peer, 8), lax.div(peer, 8), x),
            device_id_type=MESH_ID,
        ).wait_recv()
    levels = recv_a[:, 1]
    top = jnp.max(levels, axis=0)
    share = jnp.exp(levels - top[None])
    whole = jnp.sum(share, axis=0)
    send_b[:, 0] = (jnp.sum(share * recv_a[:, 0], axis=0) / whole).reshape(BATCH, 1, VDIM)
    send_b[:, 1] = (top + jnp.log(whole)).reshape(BATCH, 1, VDIM)

    def second(b, core):
        return pltpu.make_async_remote_copy(
            src_ref=send_b.at[b],
            dst_ref=recv_b.at[z],
            send_sem=b_send.at[2 * b + core],
            recv_sem=b_recv.at[z],
            device_id=(target_z, y, core, b),
            device_id_type=MESH_ID,
        )

    for b in range(BATCH):
        for core in range(2):
            is_self = jnp.logical_and(alone, jnp.logical_and(x == b, c == core))

            @pl.when(jnp.logical_not(is_self))
            def _():
                second(b, core).start()

    @pl.when(alone)
    def _():
        recv_b[z] = send_b[x]

    for k in range(NZ):

        @pl.when(jnp.logical_not(jnp.logical_and(alone, z == k)))
        def _():
            pltpu.make_async_remote_copy(
                src_ref=send_b.at[0],
                dst_ref=recv_b.at[k],
                send_sem=b_send.at[0],
                recv_sem=b_recv.at[k],
                device_id=(k, y, lax.rem(z, 2), lax.div(z, 2)),
                device_id_type=MESH_ID,
            ).wait_recv()

    levels = recv_b[:, 1]
    top = jnp.max(levels, axis=0)
    share = jnp.exp(levels - top[None])
    result = jnp.sum(share * recv_b[:, 0], axis=0) / jnp.sum(share, axis=0)
    out_ref[...] = jnp.where(c == 0, result[:, :64], result[:, 64:]).astype(BF16)

    for copy in first_copies:
        copy.wait_send()
    for b in range(BATCH):
        for core in range(2):
            is_self = jnp.logical_and(alone, jnp.logical_and(x == b, c == core))

            @pl.when(jnp.logical_not(is_self))
            def _():
                second(b, core).wait_send()


def shards(q_nope, q_rope, w_key_up, w_value_up, latent_cache, page_scale, block_table, lengths):
    hbm = pl.BlockSpec(memory_space=pl.ANY)
    dma = pltpu.SemaphoreType.DMA
    return pl.pallas_call(
        kernel,
        out_shape=jax.ShapeDtypeStruct((1, VDIM // 2), BF16),
        in_specs=[hbm] * 8,
        out_specs=pl.BlockSpec(memory_space=pltpu.VMEM),
        scratch_shapes=[
            pltpu.VMEM((BATCH, HEADS, NOPE), BF16),
            pltpu.VMEM((BATCH, HEADS, ROPE), BF16),
            pltpu.VMEM((HEADS, NOPE, LAT), BF16),
            pltpu.VMEM((HEADS, LAT, VDIM), BF16),
            pltpu.VMEM((PAGES, PAGE, LAT + ROPE), BF16),
            pltpu.SMEM((PAGES,), F32),
            pltpu.VMEM((BATCH, BLOCKS), jnp.int32),
            pltpu.SMEM((BATCH,), jnp.int32),
            pltpu.VMEM((ROWS, NOPE), F32),
            pltpu.VMEM((ROWS, ROPE), F32),
            pltpu.VMEM((ROWS, LAT), F32),
            pltpu.VMEM((PAGES * PAGE, ROWS), F32),
            pltpu.VMEM((PAGES, ROWS), F32),
            pltpu.VMEM((GROUP, 2, BATCH, VDIM), F32),
            pltpu.VMEM((GROUP, 2, BATCH, VDIM), F32),
            pltpu.VMEM((BATCH, 2, 1, VDIM), F32),
            pltpu.VMEM((NZ, 2, 1, VDIM), F32),
            dma((7,)),
            dma((CHUNKS,)),
            dma((GROUP,)),
            dma((GROUP,)),
            dma((2 * BATCH,)),
            dma((NZ,)),
        ],
        compiler_params=pltpu.CompilerParams(collective_id=0, has_side_effects=True),
        name="latent_decode",
    )(q_nope, q_rope, w_key_up, w_value_up, latent_cache, page_scale, block_table, lengths)


def solution(mesh):
    split = Mesh(
        mesh.devices.reshape(8, 8, 2, mesh.shape["head"]), ("seq_0", "seq_1", "seq_2", "head")
    )
    return jax.shard_map(
        shards,
        mesh=split,
        in_specs=(
            P(None, "head", None),
            P(None, "head", None),
            P("head", None, None),
            P("head", None, None),
            P(SEQ, None, None),
            P(SEQ),
            P(None, SEQ),
            P(),
        ),
        out_specs=P("head", SEQ),
        check_vma=False,
    )
```

```python
import jax
import jax.numpy as jnp
from jax import lax
from jax.experimental import pallas as pl
from jax.experimental.pallas import tpu as pltpu
from jax.sharding import Mesh
from jax.sharding import PartitionSpec as P

SEQ = ("seq_0", "seq_1", "seq_2")
F32 = jnp.float32
BF16 = jnp.bfloat16
MESH_ID = pl.DeviceIdType.MESH

BATCH = 4
HEADS = 16
ROWS = BATCH * HEADS
LAT = 512
ROPE = 64
NOPE = 128
VDIM = 128
HALF = VDIM // 2
PAGE = 64
PAGES = 64
BLOCKS = 16
CHUNK = 8
CHUNKS = PAGES // CHUNK
SPAN = CHUNK * PAGE
PIECES = 4
PIECE = HEADS // PIECES
SOURCES = 128
FLOOR = -1e30


def to_column(row, eye):
    return jnp.sum(jnp.where(eye, jnp.broadcast_to(row, eye.shape), 0.0), axis=1, keepdims=True)


def kernel(
    qn_hbm, qr_hbm, wk_hbm, wv_hbm, cache_hbm, ps_hbm, bt_hbm, len_hbm, out_ref,
    qn, qr, wk, wv, cache, ps, bt, ln, qs, qrs, ql, s_buf, vc, send, recv,
    in_sem, wk_sem, cache_sem, send_sem, recv_sem,
):
    z = lax.axis_index("seq_0")
    y = lax.axis_index("seq_1")
    c = lax.axis_index("seq_2")
    x = lax.axis_index("head")

    small = [
        pltpu.make_async_copy(src, dst, in_sem.at[k])
        for k, (src, dst) in enumerate(
            [(qn_hbm, qn), (qr_hbm, qr), (bt_hbm, bt), (len_hbm, ln), (ps_hbm, ps), (wv_hbm, wv)]
        )
    ]
    keys = [
        pltpu.make_async_copy(
            wk_hbm.at[pl.ds(k * PIECE, PIECE)], wk.at[pl.ds(k * PIECE, PIECE)], wk_sem.at[k]
        )
        for k in range(PIECES)
    ]
    pages = [
        pltpu.make_async_copy(
            cache_hbm.at[pl.ds(k * CHUNK, CHUNK)], cache.at[pl.ds(k * CHUNK, CHUNK)], cache_sem.at[k]
        )
        for k in range(CHUNKS)
    ]
    for copy in small[:5] + keys + pages[:2]:
        copy.start()

    me = (z * 8 + y) * 2 + c
    plane = lax.div(z, 2)
    alone = plane == x
    barrier = pltpu.get_barrier_semaphore()
    for k in range(SOURCES):
        is_self = jnp.logical_and(alone, me == k)
        core = jnp.where(is_self, 1 - k % 2, k % 2)
        pl.semaphore_signal(
            barrier, inc=1, device_id=(k // 16, (k // 2) % 8, core, plane), device_id_type=MESH_ID
        )

    for copy in small[:5]:
        copy.wait()
    for b in range(BATCH):
        qs[pl.ds(b, HEADS, stride=BATCH), :] = qn[b].astype(F32)
        qrs[pl.ds(b, HEADS, stride=BATCH), :] = qr[b].astype(F32)
    q_rope = qrs[...].astype(BF16)

    column = lax.broadcasted_iota(jnp.int32, (PAGES, ROWS), 1)
    request = lax.rem(column, BATCH)
    first = me * (BLOCKS * PAGE)
    page_id = lax.broadcasted_iota(jnp.int32, (PAGES, BLOCKS), 0)
    block = lax.broadcasted_iota(jnp.int32, (PAGES, BLOCKS), 1)
    valid = jnp.zeros((PAGES, ROWS), F32)
    for b in range(BATCH):
        left = jnp.clip(ln[b] - first - block * PAGE, 0, PAGE).astype(F32)
        owned = jnp.where(jnp.broadcast_to(bt[b : b + 1, :], (PAGES, BLOCKS)) == page_id, left, 0.0)
        valid = jnp.where(request == b, jnp.sum(owned, axis=1, keepdims=True), valid)
    vc[...] = valid

    for k in range(PIECES):
        keys[k].wait()
        if 2 + k < CHUNKS:
            pages[2 + k].start()
        for h in range(k * PIECE, (k + 1) * PIECE):
            lhs = qs[pl.ds(16 * (h // 4), 16), :].astype(BF16)
            part = jnp.dot(lhs, wk[h], preferred_element_type=F32)
            at = 4 * (h % 4)
            ql[pl.ds(4 * h, 4), :] = part[at : at + 4]
    q_lat = ql[...].astype(BF16)

    contract = (((1,), (1,)), ((), ()))
    row_id = lax.broadcasted_iota(jnp.int32, (PAGE, ROWS), 0).astype(F32)
    peak = jnp.full((PAGE, ROWS), FLOOR, F32)
    for k in range(CHUNKS):
        pages[k].wait()
        if 2 + PIECES + k < CHUNKS:
            pages[2 + PIECES + k].start()
        elif 2 + PIECES + k == CHUNKS:
            small[5].start()
        lat_rows = cache[pl.ds(k * CHUNK, CHUNK), :, :LAT].reshape(SPAN, LAT)
        rope_rows = cache[pl.ds(k * CHUNK, CHUNK), :, LAT:].reshape(SPAN, ROPE)
        raw = lax.dot_general(lat_rows, q_lat, contract, preferred_element_type=F32)
        raw = raw + lax.dot_general(rope_rows, q_rope, contract, preferred_element_type=F32)
        for i in range(CHUNK):
            p = k * CHUNK + i
            scaled = raw[i * PAGE : (i + 1) * PAGE] * (ps[p] * (NOPE + ROPE) ** (-0.5))
            score = jnp.where(row_id < vc[pl.ds(p, 1), :], scaled, FLOOR)
            s_buf[pl.ds(p * PAGE, PAGE), :] = score
            peak = jnp.maximum(peak, score)
    peak = jnp.max(peak, axis=0, keepdims=True)
    floor = jnp.maximum(peak, -1e29)

    total = jnp.zeros((PAGE, ROWS), F32)
    latent = jnp.zeros((ROWS, LAT), F32)
    for k in range(CHUNKS):
        pieces = []
        for i in range(CHUNK):
            p = k * CHUNK + i
            weight = jnp.exp(s_buf[pl.ds(p * PAGE, PAGE), :] - floor)
            total = total + weight
            pieces.append(weight * ps[p])
        prob = jnp.concatenate(pieces, axis=0).T.astype(BF16)
        lat_rows = cache[pl.ds(k * CHUNK, CHUNK), :, :LAT].reshape(SPAN, LAT)
        latent = latent + jnp.dot(prob, lat_rows, preferred_element_type=F32)
    denominator = jnp.sum(total, axis=0, keepdims=True)

    eye = lax.broadcasted_iota(jnp.int32, (ROWS, ROWS), 0) == lax.broadcasted_iota(jnp.int32, (ROWS, ROWS), 1)
    some = denominator > 0.0
    safe = jnp.where(some, denominator, 1.0)
    level = to_column(jnp.where(some, floor + jnp.log(safe), FLOOR), eye)
    inverse = to_column(1.0 / safe, eye)
    level = jnp.broadcast_to(level, (ROWS, VDIM))
    latent = (latent * inverse).astype(BF16)

    small[5].wait()
    pl.semaphore_wait(barrier, SOURCES)

    low = lax.broadcasted_iota(jnp.int32, (BATCH, VDIM), 1) < HALF
    mine = jnp.where(alone, c * ROWS + 4 * ((z - 2 * x) * 8 + y) + x, -1)
    rows = send.reshape(2 * ROWS, VDIM)
    for h in range(HEADS):
        part = jnp.dot(latent[16 * (h // 4) : 16 * (h // 4) + 16], wv[h], preferred_element_type=F32)
        at = 4 * (h % 4)
        rows[pl.ds(4 * h, 4), :] = jnp.where(low, part[at : at + 4], level[4 * h : 4 * h + 4])
        rows[pl.ds(ROWS + 4 * h, 4), :] = jnp.where(low, level[4 * h : 4 * h + 4], part[at : at + 4])
        for b in range(BATCH):
            for core in range(2):
                k = core * ROWS + 4 * h + b
                is_self = mine == k
                pltpu.make_async_remote_copy(
                    src_ref=send.at[k],
                    dst_ref=recv.at[jnp.where(is_self, SOURCES, me)],
                    send_sem=send_sem,
                    recv_sem=recv_sem,
                    device_id=(2 * x + h // 8, h % 8, jnp.where(is_self, 1 - core, core), b),
                    device_id_type=MESH_ID,
                ).start()

    pltpu.make_async_copy(recv.at[pl.ds(0, SOURCES)], recv.at[pl.ds(0, SOURCES)], recv_sem).wait()

    @pl.when(alone)
    def _():
        recv[me] = send[jnp.maximum(mine, 0)]

    gathered = recv.reshape(SOURCES + 1, VDIM)[pl.ds(0, SOURCES), :]
    top = jnp.max(gathered, axis=0, keepdims=True)
    share = pltpu.roll(jnp.exp(gathered - top), HALF, 1)
    result = jnp.sum(share * gathered, axis=0, keepdims=True) / jnp.sum(share, axis=0, keepdims=True)
    out_ref[...] = jnp.where(c == 0, result[:, :HALF], result[:, HALF:]).astype(BF16)
    pltpu.make_async_copy(send, send, send_sem).wait()


def shards(q_nope, q_rope, w_key_up, w_value_up, latent_cache, page_scale, block_table, lengths):
    hbm = pl.BlockSpec(memory_space=pl.ANY)
    dma = pltpu.SemaphoreType.DMA
    return pl.pallas_call(
        kernel,
        out_shape=pltpu.VMEM((1, HALF), BF16),
        in_specs=[hbm] * 8,
        out_specs=pl.BlockSpec(memory_space=pltpu.VMEM),
        scratch_shapes=[
            pltpu.VMEM((BATCH, HEADS, NOPE), BF16),
            pltpu.VMEM((BATCH, HEADS, ROPE), BF16),
            pltpu.VMEM((HEADS, NOPE, LAT), BF16),
            pltpu.VMEM((HEADS, LAT, VDIM), BF16),
            pltpu.VMEM((PAGES, PAGE, LAT + ROPE), BF16),
            pltpu.SMEM((PAGES,), F32),
            pltpu.VMEM((BATCH, BLOCKS), jnp.int32),
            pltpu.SMEM((BATCH,), jnp.int32),
            pltpu.VMEM((ROWS, NOPE), F32),
            pltpu.VMEM((ROWS, ROPE), F32),
            pltpu.VMEM((ROWS, LAT), F32),
            pltpu.VMEM((PAGES * PAGE, ROWS), F32),
            pltpu.VMEM((PAGES, ROWS), F32),
            pltpu.VMEM((2 * ROWS, 1, VDIM), F32),
            pltpu.VMEM((SOURCES + 1, 1, VDIM), F32),
            dma((6,)),
            dma((PIECES,)),
            dma((CHUNKS,)),
            dma,
            dma,
        ],
        compiler_params=pltpu.CompilerParams(collective_id=0, has_side_effects=True),
        name="latent_decode",
    )(q_nope, q_rope, w_key_up, w_value_up, latent_cache, page_scale, block_table, lengths)


def solution(mesh):
    split = Mesh(
        mesh.devices.reshape(8, 8, 2, mesh.shape["head"]), ("seq_0", "seq_1", "seq_2", "head")
    )
    return jax.shard_map(
        shards,
        mesh=split,
        in_specs=(
            P(None, "head", None),
            P(None, "head", None),
            P("head", None, None),
            P("head", None, None),
            P(SEQ, None, None),
            P(SEQ),
            P(None, SEQ),
            P(),
        ),
        out_specs=P("head", SEQ),
        check_vma=False,
    )
```

```python
import jax
import jax.numpy as jnp
from jax import lax
from jax.experimental import pallas as pl
from jax.experimental.pallas import tpu as pltpu
from jax.sharding import Mesh
from jax.sharding import PartitionSpec as P

SEQ = ("seq_0", "seq_1", "seq_2")
F32 = jnp.float32
BF16 = jnp.bfloat16

BATCH = 4
HEADS = 16
ROWS = BATCH * HEADS
LAT = 512
ROPE = 64
NOPE = 128
VDIM = 128
HALF = VDIM // 2
PAGE = 64
PAGES = 64
BLOCKS = 16
CHUNK = 8
CHUNKS = PAGES // CHUNK
SPAN = CHUNK * PAGE
PIECES = 4
PIECE = HEADS // PIECES
LANES = 128
SIDE = 4
PARTS = 2
TILES = SIDE * ROWS // LANES
NX = 4
EARLY = 6
UNROLL = 8
SOURCES = 128
FLOOR = -1e30


def place(rhs, first, depth, block):
    empty = jnp.zeros((depth, ROWS), BF16)
    left = jnp.concatenate([block, empty], axis=1)
    right = jnp.concatenate([empty, block], axis=1)
    for i in range(SIDE):
        rhs[pl.ds(first + i * depth, depth), pl.ds(i // 2 * LANES, LANES)] = right if i % 2 else left


def kernel(
    qn_hbm, qr_hbm, wk_hbm, wv_hbm, cache_hbm, ps_hbm, bt_hbm, len_hbm, out_ref,
    qn, qr, wk, wv, cache, ps, bt, ln, qs, qrs, ql, s_buf, vc, rhs, send, recv,
    in_sem, wk_sem, cache_sem, send_sem, recv_sem,
):
    z = lax.axis_index("seq_0")
    y = lax.axis_index("seq_1")
    c = lax.axis_index("seq_2")
    x = lax.axis_index("head")

    small = [
        pltpu.make_async_copy(src, dst, in_sem.at[k])
        for k, (src, dst) in enumerate(
            [(qn_hbm, qn), (qr_hbm, qr), (bt_hbm, bt), (len_hbm, ln), (ps_hbm, ps), (wv_hbm, wv)]
        )
    ]
    keys = [
        pltpu.make_async_copy(
            wk_hbm.at[pl.ds(k * PIECE, PIECE)], wk.at[pl.ds(k * PIECE, PIECE)], wk_sem.at[k]
        )
        for k in range(PIECES)
    ]
    pages = [
        pltpu.make_async_copy(
            cache_hbm.at[pl.ds(k * CHUNK, CHUNK)], cache.at[pl.ds(k * CHUNK, CHUNK)], cache_sem.at[k]
        )
        for k in range(CHUNKS)
    ]
    for copy in small[:5] + keys:
        copy.start()

    me = (z * 8 + y) * 2 + c
    plane = lax.div(z, 2)
    alone = plane == x
    other = me + 1 - 2 * c
    barrier = pltpu.get_barrier_semaphore()

    def greet(k):
        pl.semaphore_signal(
            barrier, inc=1, device_id=k * NX + plane, device_id_type=pl.DeviceIdType.LOGICAL
        )

    greet(jnp.where(alone, other, me))

    def greet_all(first, last):
        @pl.loop(first, last)
        def _(i):
            for j in range(1, UNROLL + 1):
                greet(lax.rem(me + i * UNROLL + j, SOURCES))

    greet_all(0, EARLY)
    for copy in pages[:SIDE]:
        copy.start()
    greet_all(EARLY, SOURCES // UNROLL - 1)
    for j in range(1, UNROLL):
        greet(lax.rem(me + SOURCES - UNROLL + j, SOURCES))
    for copy in pages[SIDE:]:
        copy.start()

    for copy in small[:5]:
        copy.wait()
    for b in range(BATCH):
        qs[pl.ds(b, HEADS, stride=BATCH), :] = qn[b].astype(F32)
        qrs[pl.ds(b, HEADS, stride=BATCH), :] = qr[b].astype(F32)

    request = lax.rem(lax.broadcasted_iota(jnp.int32, (PAGES, ROWS), 1), BATCH)
    page_id = lax.broadcasted_iota(jnp.int32, (PAGES, BLOCKS), 0)
    block = lax.broadcasted_iota(jnp.int32, (PAGES, BLOCKS), 1)
    valid = jnp.zeros((PAGES, ROWS), F32)
    for b in range(BATCH):
        left = jnp.clip(ln[b] - (me * BLOCKS + block) * PAGE, 0, PAGE).astype(F32)
        owned = jnp.where(jnp.broadcast_to(bt[b : b + 1, :], (PAGES, BLOCKS)) == page_id, left, 0.0)
        valid = jnp.where(request == b, jnp.sum(owned, axis=1, keepdims=True), valid)
    for g in range(PAGES // 16):
        vc[g] = jnp.concatenate([valid[16 * g : 16 * g + 8], valid[16 * g + 8 : 16 * g + 16]], axis=1)
    rhs[...] = jnp.zeros((SIDE * (LAT + ROPE), SIDE * ROWS), BF16)
    place(rhs, SIDE * LAT, ROPE, qrs[...].T.astype(BF16))

    for k in range(PIECES):
        keys[k].wait()
        for h in range(k * PIECE, (k + 1) * PIECE):
            lhs = qs[pl.ds(16 * (h // 4), 16), :].astype(BF16)
            part = jnp.dot(lhs, wk[h], preferred_element_type=F32)
            at = 4 * (h % 4)
            ql[pl.ds(4 * h, 4), :] = part[at : at + 4]
    place(rhs, 0, LAT, ql[...].T.astype(BF16))

    small[5].start()
    row_id = lax.broadcasted_iota(jnp.int32, (PAGE, LANES), 0).astype(F32)
    even = lax.broadcasted_iota(jnp.int32, (1, LANES), 1) < ROWS

    def scale_of(s, tile, page):
        p = (s * SIDE + 2 * tile) * CHUNK + page
        return jnp.where(even, ps[p], ps[p + CHUNK])

    def scores(s):
        for i in range(SIDE):
            pages[s * SIDE + i].wait()
        raw = []
        for part in range(PARTS):
            first = part * (CHUNK // PARTS)
            here = [pl.ds((s * SIDE + i) * CHUNK + first, CHUNK // PARTS) for i in range(SIDE)]
            lhs = [cache[at, :, :LAT].reshape(SPAN // PARTS, LAT) for at in here]
            lhs = lhs + [cache[at, :, LAT:].reshape(SPAN // PARTS, ROPE) for at in here]
            raw.append(jnp.dot(jnp.concatenate(lhs, axis=1), rhs[...], preferred_element_type=F32))
        peak = jnp.full((PAGE, LANES), FLOOR, F32)
        for page in range(CHUNK):
            for tile in range(TILES):
                scale = scale_of(s, tile, page) * (NOPE + ROPE) ** (-0.5)
                at = page % (CHUNK // PARTS) * PAGE
                scaled = raw[page // (CHUNK // PARTS)][at : at + PAGE, tile * LANES : (tile + 1) * LANES] * scale
                score = jnp.where(row_id < vc[s * TILES + tile, pl.ds(page, 1), :], scaled, FLOOR)
                s_buf[s, tile, pl.ds(page * PAGE, PAGE), :] = score
                peak = jnp.maximum(peak, score)
        peak = jnp.max(peak, axis=0, keepdims=True)
        return jnp.maximum(peak, pltpu.roll(peak, ROWS, 1))

    def weighted(s, floor):
        total = jnp.zeros((PAGE, LANES), F32)
        latent = [jnp.zeros((ROWS, LAT // PARTS), F32) for _ in range(PARTS)]
        for tile in range(TILES):
            pieces = []
            for page in range(CHUNK):
                weight = jnp.exp(s_buf[s, tile, pl.ds(page * PAGE, PAGE), :] - floor)
                total = total + weight
                pieces.append(weight * scale_of(s, tile, page))
            prob = jnp.concatenate(pieces, axis=0).T.astype(BF16)
            for i in range(2):
                k = s * SIDE + 2 * tile + i
                for part in range(PARTS):
                    columns = pl.ds(part * (LAT // PARTS), LAT // PARTS)
                    lat_rows = cache[pl.ds(k * CHUNK, CHUNK), :, columns].reshape(SPAN, LAT // PARTS)
                    latent[part] = latent[part] + jnp.dot(
                        prob[i * ROWS : (i + 1) * ROWS], lat_rows, preferred_element_type=F32
                    )
        total = jnp.sum(total, axis=0, keepdims=True)
        return total + pltpu.roll(total, ROWS, 1), jnp.concatenate(latent, axis=1)

    former = jnp.maximum(scores(0), -1e29)
    floor = jnp.maximum(scores(1), former)
    total, latent = weighted(0, former)
    total_two, latent_two = weighted(1, floor)
    correction = jnp.exp(former - floor)
    denominator = total * correction + total_two

    some = denominator > 0.0
    safe = jnp.where(some, denominator, 1.0)
    level = jnp.where(some, floor + jnp.log(safe), FLOOR)
    sub = lax.broadcasted_iota(jnp.int32, (8, LANES), 0)
    inverse = 1.0 / safe
    columns = jnp.where(sub == 0, level, jnp.where(sub == 1, inverse, correction * inverse)).T
    level = jnp.broadcast_to(columns[:ROWS, 0:1], (ROWS, VDIM))
    latent = (latent * columns[:ROWS, 2:3] + latent_two * columns[:ROWS, 1:2]).astype(BF16)

    small[5].wait()
    pl.semaphore_wait(barrier, SOURCES)
    sub = lax.broadcasted_iota(jnp.int32, (8, VDIM), 0)
    low = lax.broadcasted_iota(jnp.int32, (8, VDIM), 1) < HALF
    data_lane = (sub < BATCH) == low
    rows = send.reshape(2 * ROWS, VDIM)
    mine = lax.rem(me * NX + x, SOURCES)

    def post(t, slot, to):
        pltpu.make_async_remote_copy(
            src_ref=send.at[t],
            dst_ref=recv.at[slot],
            send_sem=send_sem,
            recv_sem=recv_sem,
            device_id=to,
            device_id_type=pl.DeviceIdType.LOGICAL,
        ).start()

    def project(h):
        part = jnp.dot(latent[16 * (h // 4) : 16 * (h // 4) + 16], wv[h], preferred_element_type=F32)
        at = 4 * (h % 4)
        part = part[at : at + 4]
        mark = level[4 * h : 4 * h + 4]
        rows[pl.ds(8 * h, 8), :] = jnp.where(
            data_lane, jnp.concatenate([part, part], axis=0), jnp.concatenate([mark, mark], axis=0)
        )

    project(0)
    for t in range(8):
        is_self = jnp.logical_and(alone, mine == t)
        post(t, jnp.where(is_self, SOURCES, me), SOURCES * x + jnp.where(is_self, t ^ NX, t))
    for h in range(1, HEADS):
        project(h)

    @pl.loop(1, SOURCES // UNROLL)
    def _(i):
        for j in range(UNROLL):
            t = i * UNROLL + j
            is_self = jnp.logical_and(alone, mine == t)
            turned = SOURCES * x + t + jnp.where(is_self, NX * (1 - 2 * c), 0)
            post(t, jnp.where(is_self, SOURCES, me), turned)

    pltpu.make_async_copy(recv.at[pl.ds(0, SOURCES)], recv.at[pl.ds(0, SOURCES)], recv_sem).wait()

    @pl.when(alone)
    def _():
        recv[me] = send[mine]

    gathered = recv.reshape(SOURCES + 1, VDIM)[pl.ds(0, SOURCES), :]
    top = jnp.max(gathered, axis=0, keepdims=True)
    share = pltpu.roll(jnp.exp(gathered - top), HALF, 1)
    result = jnp.sum(share * gathered, axis=0, keepdims=True) / jnp.sum(share, axis=0, keepdims=True)
    out_ref[...] = jnp.where(c == 0, result[:, :HALF], result[:, HALF:]).astype(BF16)
    pltpu.make_async_copy(send, send, send_sem).wait()


def shards(q_nope, q_rope, w_key_up, w_value_up, latent_cache, page_scale, block_table, lengths):
    hbm = pl.BlockSpec(memory_space=pl.ANY)
    dma = pltpu.SemaphoreType.DMA
    return pl.pallas_call(
        kernel,
        out_shape=pltpu.VMEM((1, HALF), BF16),
        in_specs=[hbm] * 8,
        out_specs=pl.BlockSpec(memory_space=pltpu.VMEM),
        scratch_shapes=[
            pltpu.VMEM((BATCH, HEADS, NOPE), BF16),
            pltpu.VMEM((BATCH, HEADS, ROPE), BF16),
            pltpu.VMEM((HEADS, NOPE, LAT), BF16),
            pltpu.VMEM((HEADS, LAT, VDIM), BF16),
            pltpu.VMEM((PAGES, PAGE, LAT + ROPE), BF16),
            pltpu.SMEM((PAGES,), F32),
            pltpu.VMEM((BATCH, BLOCKS), jnp.int32),
            pltpu.SMEM((BATCH,), jnp.int32),
            pltpu.VMEM((ROWS, NOPE), F32),
            pltpu.VMEM((ROWS, ROPE), F32),
            pltpu.VMEM((ROWS, LAT), F32),
            pltpu.VMEM((CHUNKS // SIDE, TILES, SPAN, LANES), F32),
            pltpu.VMEM((PAGES // 16, 8, LANES), F32),
            pltpu.VMEM((SIDE * (LAT + ROPE), SIDE * ROWS), BF16),
            pltpu.VMEM((2 * ROWS, 1, VDIM), F32),
            pltpu.VMEM((SOURCES + 1, 1, VDIM), F32),
            dma((6,)),
            dma((PIECES,)),
            dma((CHUNKS,)),
            dma,
            dma,
        ],
        compiler_params=pltpu.CompilerParams(collective_id=0, has_side_effects=True),
        name="latent_decode",
    )(q_nope, q_rope, w_key_up, w_value_up, latent_cache, page_scale, block_table, lengths)


def solution(mesh):
    split = Mesh(
        mesh.devices.reshape(8, 8, 2, mesh.shape["head"]), ("seq_0", "seq_1", "seq_2", "head")
    )
    return jax.shard_map(
        shards,
        mesh=split,
        in_specs=(
            P(None, "head", None),
            P(None, "head", None),
            P("head", None, None),
            P("head", None, None),
            P(SEQ, None, None),
            P(SEQ),
            P(None, SEQ),
            P(),
        ),
        out_specs=P("head", SEQ),
        check_vma=False,
    )
```

```python
import jax
import jax.numpy as jnp
from jax import lax
from jax.experimental import pallas as pl
from jax.experimental.pallas import tpu as pltpu
from jax.sharding import Mesh
from jax.sharding import PartitionSpec as P

SEQ = ("seq_0", "seq_1", "seq_2")
F32 = jnp.float32
BF16 = jnp.bfloat16

BATCH = 4
HEADS = 16
ROWS = BATCH * HEADS
LAT = 512
ROPE = 64
NOPE = 128
VDIM = 128
HALF = VDIM // 2
PAGE = 64
PAGES = 64
BLOCKS = 16
CHUNK = 8
CHUNKS = PAGES // CHUNK
SPAN = CHUNK * PAGE
PIECES = 4
PIECE = HEADS // PIECES
LANES = 128
SIDE = 4
PARTS = 2
TILES = SIDE * ROWS // LANES
NX = 4
EARLY = 4
LATE = 11
UNROLL = 8
SOURCES = 128
FLOOR = -1e30


def place(rhs, first, depth, block):
    empty = jnp.zeros((depth, ROWS), BF16)
    left = jnp.concatenate([block, empty], axis=1)
    right = jnp.concatenate([empty, block], axis=1)
    for i in range(SIDE):
        rhs[pl.ds(first + i * depth, depth), pl.ds(i // 2 * LANES, LANES)] = right if i % 2 else left


def kernel(
    qn_hbm, qr_hbm, wk_hbm, wv_hbm, cache_hbm, ps_hbm, bt_hbm, len_hbm, out_ref,
    qn, qr, wk, wv, cache, ps, bt, ln, qs, qrs, ql, s_buf, vc, rhs, send, recv,
    in_sem, wk_sem, cache_sem, send_sem, recv_sem,
):
    z = lax.axis_index("seq_0")
    y = lax.axis_index("seq_1")
    c = lax.axis_index("seq_2")
    x = lax.axis_index("head")

    small = [
        pltpu.make_async_copy(src, dst, in_sem.at[k])
        for k, (src, dst) in enumerate(
            [(qn_hbm, qn), (qr_hbm, qr), (bt_hbm, bt), (len_hbm, ln), (ps_hbm, ps), (wv_hbm, wv)]
        )
    ]
    keys = [
        pltpu.make_async_copy(
            wk_hbm.at[pl.ds(k * PIECE, PIECE)], wk.at[pl.ds(k * PIECE, PIECE)], wk_sem.at[k]
        )
        for k in range(PIECES)
    ]
    pages = [
        pltpu.make_async_copy(
            cache_hbm.at[pl.ds(k * CHUNK, CHUNK)], cache.at[pl.ds(k * CHUNK, CHUNK)], cache_sem.at[k]
        )
        for k in range(CHUNKS)
    ]
    for copy in small[:5] + keys:
        copy.start()

    rhs[...] = jnp.zeros((SIDE * (LAT + ROPE), SIDE * ROWS), BF16)

    me = (z * 8 + y) * 2 + c
    plane = lax.div(z, 2)
    alone = plane == x
    other = me + 1 - 2 * c
    barrier = pltpu.get_barrier_semaphore()

    def greet(k):
        pl.semaphore_signal(
            barrier, inc=1, device_id=k * NX + plane, device_id_type=pl.DeviceIdType.LOGICAL
        )

    greet(jnp.where(alone, other, me))

    def greet_all(first, last):
        @pl.loop(first, last)
        def _(i):
            for j in range(1, UNROLL + 1):
                greet(lax.rem(me + i * UNROLL + j, SOURCES))

    greet_all(0, EARLY)
    for copy in pages[:SIDE]:
        copy.start()
    greet_all(EARLY, LATE)
    for copy in pages[SIDE:]:
        copy.start()
    greet_all(LATE, SOURCES // UNROLL - 1)
    for j in range(1, UNROLL):
        greet(lax.rem(me + SOURCES - UNROLL + j, SOURCES))

    for copy in small[:5] + keys:
        copy.wait()
    for b in range(BATCH):
        qs[pl.ds(b, HEADS, stride=BATCH), :] = qn[b].astype(F32)
        qrs[pl.ds(b, HEADS, stride=BATCH), :] = qr[b].astype(F32)

    request = lax.rem(lax.broadcasted_iota(jnp.int32, (PAGES, ROWS), 1), BATCH)
    page_id = lax.broadcasted_iota(jnp.int32, (PAGES, BLOCKS), 0)
    block = lax.broadcasted_iota(jnp.int32, (PAGES, BLOCKS), 1)
    valid = jnp.zeros((PAGES, ROWS), F32)
    for b in range(BATCH):
        left = jnp.clip(ln[b] - (me * BLOCKS + block) * PAGE, 0, PAGE).astype(F32)
        owned = jnp.where(jnp.broadcast_to(bt[b : b + 1, :], (PAGES, BLOCKS)) == page_id, left, 0.0)
        valid = jnp.where(request == b, jnp.sum(owned, axis=1, keepdims=True), valid)
    for g in range(PAGES // 16):
        vc[g] = jnp.concatenate([valid[16 * g : 16 * g + 8], valid[16 * g + 8 : 16 * g + 16]], axis=1)
    place(rhs, SIDE * LAT, ROPE, qrs[...].T.astype(BF16))

    for h in range(HEADS):
        lhs = qs[pl.ds(16 * (h // 4), 16), :].astype(BF16)
        part = jnp.dot(lhs, wk[h], preferred_element_type=F32)
        at = 4 * (h % 4)
        ql[pl.ds(4 * h, 4), :] = part[at : at + 4]
    place(rhs, 0, LAT, ql[...].T.astype(BF16))

    small[5].start()
    row_id = lax.broadcasted_iota(jnp.int32, (PAGE, LANES), 0).astype(F32)
    even = lax.broadcasted_iota(jnp.int32, (1, LANES), 1) < ROWS

    def scale_of(s, tile, page):
        p = (s * SIDE + 2 * tile) * CHUNK + page
        return jnp.where(even, ps[p], ps[p + CHUNK])

    def products(s):
        for i in range(SIDE):
            pages[s * SIDE + i].wait()
        raw = []
        for part in range(PARTS):
            first = part * (CHUNK // PARTS)
            here = [pl.ds((s * SIDE + i) * CHUNK + first, CHUNK // PARTS) for i in range(SIDE)]
            lhs = [cache[at, :, :LAT].reshape(SPAN // PARTS, LAT) for at in here]
            lhs = lhs + [cache[at, :, LAT:].reshape(SPAN // PARTS, ROPE) for at in here]
            raw.append(jnp.dot(jnp.concatenate(lhs, axis=1), rhs[...], preferred_element_type=F32))
        return raw

    def scores(s, raw):
        peak = jnp.full((PAGE, LANES), FLOOR, F32)
        for page in range(CHUNK):
            for tile in range(TILES):
                scale = scale_of(s, tile, page) * (NOPE + ROPE) ** (-0.5)
                at = page % (CHUNK // PARTS) * PAGE
                scaled = raw[page // (CHUNK // PARTS)][at : at + PAGE, tile * LANES : (tile + 1) * LANES] * scale
                score = jnp.where(row_id < vc[s * TILES + tile, pl.ds(page, 1), :], scaled, FLOOR)
                s_buf[s, tile, pl.ds(page * PAGE, PAGE), :] = score
                peak = jnp.maximum(peak, score)
        peak = jnp.max(peak, axis=0, keepdims=True)
        return jnp.maximum(peak, pltpu.roll(peak, ROWS, 1))

    def weighted(s, floor):
        total = jnp.zeros((PAGE, LANES), F32)
        latent = [jnp.zeros((ROWS, LAT // PARTS), F32) for _ in range(PARTS)]
        for tile in range(TILES):
            pieces = []
            for page in range(CHUNK):
                weight = jnp.exp(s_buf[s, tile, pl.ds(page * PAGE, PAGE), :] - floor)
                total = total + weight
                pieces.append(weight * scale_of(s, tile, page))
            prob = jnp.concatenate(pieces, axis=0).T.astype(BF16)
            for i in range(2):
                k = s * SIDE + 2 * tile + i
                for part in range(PARTS):
                    columns = pl.ds(part * (LAT // PARTS), LAT // PARTS)
                    lat_rows = cache[pl.ds(k * CHUNK, CHUNK), :, columns].reshape(SPAN, LAT // PARTS)
                    latent[part] = latent[part] + jnp.dot(
                        prob[i * ROWS : (i + 1) * ROWS], lat_rows, preferred_element_type=F32
                    )
        total = jnp.sum(total, axis=0, keepdims=True)
        return total + pltpu.roll(total, ROWS, 1), jnp.concatenate(latent, axis=1)

    raw = [products(s) for s in range(CHUNKS // SIDE)]
    former = jnp.maximum(scores(0, raw[0]), -1e29)
    floor = jnp.maximum(scores(1, raw[1]), former)
    total, latent = weighted(0, former)
    total_two, latent_two = weighted(1, floor)
    correction = jnp.exp(former - floor)
    denominator = total * correction + total_two

    some = denominator > 0.0
    safe = jnp.where(some, denominator, 1.0)
    level = jnp.where(some, floor + jnp.log(safe), FLOOR)
    sub = lax.broadcasted_iota(jnp.int32, (8, LANES), 0)
    inverse = 1.0 / safe
    columns = jnp.where(sub == 0, level, jnp.where(sub == 1, inverse, correction * inverse)).T
    level = jnp.broadcast_to(columns[:ROWS, 0:1], (ROWS, VDIM))
    latent = (latent * columns[:ROWS, 2:3] + latent_two * columns[:ROWS, 1:2]).astype(BF16)

    small[5].wait()
    pl.semaphore_wait(barrier, SOURCES)
    sub = lax.broadcasted_iota(jnp.int32, (8, VDIM), 0)
    low = lax.broadcasted_iota(jnp.int32, (8, VDIM), 1) < HALF
    data_lane = (sub < BATCH) == low
    rows = send.reshape(2 * ROWS, VDIM)
    mine = lax.rem(me * NX + x, SOURCES)

    def post(t, slot, to):
        pltpu.make_async_remote_copy(
            src_ref=send.at[t],
            dst_ref=recv.at[slot],
            send_sem=send_sem,
            recv_sem=recv_sem,
            device_id=to,
            device_id_type=pl.DeviceIdType.LOGICAL,
        ).start()

    def project(h):
        part = jnp.dot(latent[16 * (h // 4) : 16 * (h // 4) + 16], wv[h], preferred_element_type=F32)
        at = 4 * (h % 4)
        part = part[at : at + 4]
        mark = level[4 * h : 4 * h + 4]
        rows[pl.ds(8 * h, 8), :] = jnp.where(
            data_lane, jnp.concatenate([part, part], axis=0), jnp.concatenate([mark, mark], axis=0)
        )

    project(0)
    for t in range(8):
        is_self = jnp.logical_and(alone, mine == t)
        post(t, jnp.where(is_self, SOURCES, me), SOURCES * x + jnp.where(is_self, t ^ NX, t))
    for h in range(1, HEADS):
        project(h)

    @pl.loop(1, SOURCES // UNROLL)
    def _(i):
        for j in range(UNROLL):
            t = i * UNROLL + j
            is_self = jnp.logical_and(alone, mine == t)
            turned = SOURCES * x + t + jnp.where(is_self, NX * (1 - 2 * c), 0)
            post(t, jnp.where(is_self, SOURCES, me), turned)

    @pl.when(alone)
    def _():
        recv[me] = send[mine]

    pltpu.make_async_copy(recv.at[pl.ds(0, SOURCES)], recv.at[pl.ds(0, SOURCES)], recv_sem).wait()

    gathered = recv.reshape(SOURCES + 1, VDIM)[pl.ds(0, SOURCES), :]
    turned = pltpu.roll(gathered, HALF, 1)
    marks = jnp.where(c == 0, turned, gathered)
    share = jnp.exp(marks - jnp.max(marks, axis=0, keepdims=True))
    share_of = share * jnp.where(c == 0, gathered, turned)
    result = jnp.sum(share_of, axis=0, keepdims=True) / jnp.sum(share, axis=0, keepdims=True)
    out_ref[...] = result[:, :HALF].astype(BF16)
    pltpu.make_async_copy(send, send, send_sem).wait()


def shards(q_nope, q_rope, w_key_up, w_value_up, latent_cache, page_scale, block_table, lengths):
    hbm = pl.BlockSpec(memory_space=pl.ANY)
    dma = pltpu.SemaphoreType.DMA
    return pl.pallas_call(
        kernel,
        out_shape=pltpu.VMEM((1, HALF), BF16),
        in_specs=[hbm] * 8,
        out_specs=pl.BlockSpec(memory_space=pltpu.VMEM),
        scratch_shapes=[
            pltpu.VMEM((BATCH, HEADS, NOPE), BF16),
            pltpu.VMEM((BATCH, HEADS, ROPE), BF16),
            pltpu.VMEM((HEADS, NOPE, LAT), BF16),
            pltpu.VMEM((HEADS, LAT, VDIM), BF16),
            pltpu.VMEM((PAGES, PAGE, LAT + ROPE), BF16),
            pltpu.SMEM((PAGES,), F32),
            pltpu.VMEM((BATCH, BLOCKS), jnp.int32),
            pltpu.SMEM((BATCH,), jnp.int32),
            pltpu.VMEM((ROWS, NOPE), F32),
            pltpu.VMEM((ROWS, ROPE), F32),
            pltpu.VMEM((ROWS, LAT), F32),
            pltpu.VMEM((CHUNKS // SIDE, TILES, SPAN, LANES), F32),
            pltpu.VMEM((PAGES // 16, 8, LANES), F32),
            pltpu.VMEM((SIDE * (LAT + ROPE), SIDE * ROWS), BF16),
            pltpu.VMEM((2 * ROWS, 1, VDIM), F32),
            pltpu.VMEM((SOURCES + 1, 1, VDIM), F32),
            dma((6,)),
            dma((PIECES,)),
            dma((CHUNKS,)),
            dma,
            dma,
        ],
        compiler_params=pltpu.CompilerParams(collective_id=0, has_side_effects=True),
        name="latent_decode",
    )(q_nope, q_rope, w_key_up, w_value_up, latent_cache, page_scale, block_table, lengths)


def solution(mesh):
    split = Mesh(
        mesh.devices.reshape(8, 8, 2, mesh.shape["head"]), ("seq_0", "seq_1", "seq_2", "head")
    )
    return jax.shard_map(
        shards,
        mesh=split,
        in_specs=(
            P(None, "head", None),
            P(None, "head", None),
            P("head", None, None),
            P("head", None, None),
            P(SEQ, None, None),
            P(SEQ),
            P(None, SEQ),
            P(),
        ),
        out_specs=P("head", SEQ),
        check_vma=False,
    )
```

```python
import jax
import jax.numpy as jnp
from jax import lax
from jax.experimental import pallas as pl
from jax.experimental.pallas import tpu as pltpu
from jax.sharding import Mesh
from jax.sharding import PartitionSpec as P

SEQ = ("seq_0", "seq_1", "seq_2")
F32 = jnp.float32
BF16 = jnp.bfloat16

BATCH = 4
HEADS = 16
ROWS = BATCH * HEADS
LAT = 512
ROPE = 64
NOPE = 128
VDIM = 128
HALF = VDIM // 2
PAGE = 64
PAGES = 64
BLOCKS = 16
CHUNK = 8
CHUNKS = PAGES // CHUNK
SPAN = CHUNK * PAGE
PIECES = 4
PIECE = HEADS // PIECES
LANES = 128
SIDE = 4
PARTS = 2
TILES = 2
NX = 4
EARLY = 4
LATE = 11
UNROLL = 8
SOURCES = 128
FLOOR = -1e30


def place(rhs, first, depth, block):
    empty = jnp.zeros((depth, ROWS), BF16)
    rhs[pl.ds(first, depth), :] = jnp.concatenate([block, empty], axis=1)
    rhs[pl.ds(first + depth, depth), :] = jnp.concatenate([empty, block], axis=1)


def kernel(
    qn_hbm, qr_hbm, wk_hbm, wv_hbm, cache_hbm, ps_hbm, bt_hbm, len_hbm, out_ref,
    qn, qr, wk, wv, cache, ps, bt, ln, qs, qrs, ql, s_buf, vc, rhs, send, recv,
    in_sem, wk_sem, cache_sem, send_sem, recv_sem,
):
    z = lax.axis_index("seq_0")
    y = lax.axis_index("seq_1")
    c = lax.axis_index("seq_2")
    x = lax.axis_index("head")

    small = [
        pltpu.make_async_copy(src, dst, in_sem.at[k])
        for k, (src, dst) in enumerate(
            [(qn_hbm, qn), (qr_hbm, qr), (bt_hbm, bt), (len_hbm, ln), (ps_hbm, ps), (wv_hbm, wv)]
        )
    ]
    keys = [
        pltpu.make_async_copy(
            wk_hbm.at[pl.ds(k * PIECE, PIECE)], wk.at[pl.ds(k * PIECE, PIECE)], wk_sem.at[k]
        )
        for k in range(PIECES)
    ]
    pages = [
        pltpu.make_async_copy(
            cache_hbm.at[pl.ds(k * CHUNK, CHUNK)], cache.at[pl.ds(k * CHUNK, CHUNK)], cache_sem.at[k]
        )
        for k in range(CHUNKS)
    ]
    for copy in small[:5] + keys:
        copy.start()

    me = (z * 8 + y) * 2 + c
    plane = lax.div(z, 2)
    alone = plane == x
    other = me + 1 - 2 * c
    barrier = pltpu.get_barrier_semaphore()

    def greet(k):
        pl.semaphore_signal(
            barrier, inc=1, device_id=k * NX + plane, device_id_type=pl.DeviceIdType.LOGICAL
        )

    greet(jnp.where(alone, other, me))

    def greet_all(first, last):
        @pl.loop(first, last)
        def _(i):
            for j in range(1, UNROLL + 1):
                greet(lax.rem(me + i * UNROLL + j, SOURCES))

    greet_all(0, EARLY)
    for copy in pages[:SIDE]:
        copy.start()
    greet_all(EARLY, LATE)
    for copy in pages[SIDE:]:
        copy.start()
    greet_all(LATE, SOURCES // UNROLL - 1)
    for j in range(1, UNROLL):
        greet(lax.rem(me + SOURCES - UNROLL + j, SOURCES))

    for copy in small[:5] + keys:
        copy.wait()
    for b in range(BATCH):
        qs[pl.ds(b, HEADS, stride=BATCH), :] = qn[b].astype(F32)
        qrs[pl.ds(b, HEADS, stride=BATCH), :] = qr[b].astype(F32)

    request = lax.rem(lax.broadcasted_iota(jnp.int32, (PAGES, ROWS), 1), BATCH)
    page_id = lax.broadcasted_iota(jnp.int32, (PAGES, BLOCKS), 0)
    block = lax.broadcasted_iota(jnp.int32, (PAGES, BLOCKS), 1)
    valid = jnp.zeros((PAGES, ROWS), F32)
    for b in range(BATCH):
        left = jnp.clip(ln[b] - (me * BLOCKS + block) * PAGE, 0, PAGE).astype(F32)
        owned = jnp.where(jnp.broadcast_to(bt[b : b + 1, :], (PAGES, BLOCKS)) == page_id, left, 0.0)
        valid = jnp.where(request == b, jnp.sum(owned, axis=1, keepdims=True), valid)
    for g in range(PAGES // 16):
        vc[g] = jnp.concatenate([valid[16 * g : 16 * g + 8], valid[16 * g + 8 : 16 * g + 16]], axis=1)
    place(rhs, 2 * LAT, ROPE, qrs[...].T.astype(BF16))

    for h in range(HEADS):
        lhs = qs[pl.ds(16 * (h // 4), 16), :].astype(BF16)
        part = jnp.dot(lhs, wk[h], preferred_element_type=F32)
        at = 4 * (h % 4)
        ql[pl.ds(4 * h, 4), :] = part[at : at + 4]
    place(rhs, 0, LAT, ql[...].T.astype(BF16))

    small[5].start()
    row_id = lax.broadcasted_iota(jnp.int32, (PAGE, LANES), 0).astype(F32)
    even = lax.broadcasted_iota(jnp.int32, (1, LANES), 1) < ROWS

    def scale_of(s, tile, page):
        p = (s * SIDE + 2 * tile) * CHUNK + page
        return jnp.where(even, ps[p], ps[p + CHUNK])

    def products(s):
        for i in range(SIDE):
            pages[s * SIDE + i].wait()
        raw = []
        for tile in range(TILES):
            here = [pl.ds((s * SIDE + 2 * tile + i) * CHUNK, CHUNK) for i in range(2)]
            lhs = [cache[at, :, :LAT].reshape(SPAN, LAT) for at in here]
            lhs = lhs + [cache[at, :, LAT:].reshape(SPAN, ROPE) for at in here]
            lhs = jnp.concatenate(lhs, axis=1)
            halves = [lhs[: SPAN // 2], lhs[SPAN // 2 :]]
            raw.append(
                jnp.concatenate([jnp.dot(m, rhs[...], preferred_element_type=F32) for m in halves], axis=0)
            )
        return raw

    def scores(s, raw):
        peak = jnp.full((PAGE, LANES), FLOOR, F32)
        for page in range(CHUNK):
            for tile in range(TILES):
                scale = scale_of(s, tile, page) * (NOPE + ROPE) ** (-0.5)
                scaled = raw[tile][page * PAGE : (page + 1) * PAGE] * scale
                score = jnp.where(row_id < vc[s * TILES + tile, pl.ds(page, 1), :], scaled, FLOOR)
                s_buf[s, tile, pl.ds(page * PAGE, PAGE), :] = score
                peak = jnp.maximum(peak, score)
        peak = jnp.max(peak, axis=0, keepdims=True)
        return jnp.maximum(peak, pltpu.roll(peak, ROWS, 1))

    def weighted(s, floor):
        total = jnp.zeros((PAGE, LANES), F32)
        latent = [jnp.zeros((ROWS, LAT // PARTS), F32) for _ in range(PARTS)]
        for tile in range(TILES):
            pieces = []
            for page in range(CHUNK):
                weight = jnp.exp(s_buf[s, tile, pl.ds(page * PAGE, PAGE), :] - floor)
                total = total + weight
                pieces.append(weight * scale_of(s, tile, page))
            prob = jnp.concatenate(pieces, axis=0).T.astype(BF16)
            for i in range(2):
                k = s * SIDE + 2 * tile + i
                for part in range(PARTS):
                    columns = pl.ds(part * (LAT // PARTS), LAT // PARTS)
                    lat_rows = cache[pl.ds(k * CHUNK, CHUNK), :, columns].reshape(SPAN, LAT // PARTS)
                    latent[part] = latent[part] + jnp.dot(
                        prob[i * ROWS : (i + 1) * ROWS], lat_rows, preferred_element_type=F32
                    )
        total = jnp.sum(total, axis=0, keepdims=True)
        return total + pltpu.roll(total, ROWS, 1), jnp.concatenate(latent, axis=1)

    raw = [products(s) for s in range(CHUNKS // SIDE)]
    former = jnp.maximum(scores(0, raw[0]), -1e29)
    floor = jnp.maximum(scores(1, raw[1]), former)
    total, latent = weighted(0, former)
    total_two, latent_two = weighted(1, floor)
    correction = jnp.exp(former - floor)
    denominator = total * correction + total_two

    some = denominator > 0.0
    safe = jnp.where(some, denominator, 1.0)
    level = jnp.where(some, floor + jnp.log(safe), FLOOR)
    sub = lax.broadcasted_iota(jnp.int32, (8, LANES), 0)
    inverse = 1.0 / safe
    columns = jnp.where(sub == 0, level, jnp.where(sub == 1, inverse, correction * inverse)).T
    level = jnp.broadcast_to(columns[:ROWS, 0:1], (ROWS, VDIM))
    latent = (latent * columns[:ROWS, 2:3] + latent_two * columns[:ROWS, 1:2]).astype(BF16)

    small[5].wait()
    pl.semaphore_wait(barrier, SOURCES)
    sub = lax.broadcasted_iota(jnp.int32, (8, VDIM), 0)
    low = lax.broadcasted_iota(jnp.int32, (8, VDIM), 1) < HALF
    data_lane = (sub < BATCH) == low
    rows = send.reshape(2 * ROWS, VDIM)
    mine = lax.rem(me * NX + x, SOURCES)

    def post(t, slot, to):
        pltpu.make_async_remote_copy(
            src_ref=send.at[t],
            dst_ref=recv.at[slot],
            send_sem=send_sem,
            recv_sem=recv_sem,
            device_id=to,
            device_id_type=pl.DeviceIdType.LOGICAL,
        ).start()

    def project(h):
        part = jnp.dot(latent[16 * (h // 4) : 16 * (h // 4) + 16], wv[h], preferred_element_type=F32)
        at = 4 * (h % 4)
        part = part[at : at + 4]
        mark = level[4 * h : 4 * h + 4]
        rows[pl.ds(8 * h, 8), :] = jnp.where(
            data_lane, jnp.concatenate([part, part], axis=0), jnp.concatenate([mark, mark], axis=0)
        )

    project(0)
    for t in (4, 5, 6, 7, 0, 1, 2, 3):
        is_self = jnp.logical_and(alone, mine == t)
        post(t, jnp.where(is_self, SOURCES, me), SOURCES * x + jnp.where(is_self, t ^ NX, t))
    for h in range(1, HEADS):
        project(h)

    @pl.loop(1, SOURCES // UNROLL)
    def _(i):
        for j in range(UNROLL):
            t = i * UNROLL + j
            is_self = jnp.logical_and(alone, mine == t)
            turned = SOURCES * x + t + jnp.where(is_self, NX * (1 - 2 * c), 0)
            post(t, jnp.where(is_self, SOURCES, me), turned)

    @pl.when(alone)
    def _():
        recv[me] = send[mine]

    pltpu.make_async_copy(recv.at[pl.ds(0, SOURCES)], recv.at[pl.ds(0, SOURCES)], recv_sem).wait()

    gathered = recv.reshape(SOURCES + 1, VDIM)[pl.ds(0, SOURCES), :]
    turned = pltpu.roll(gathered, HALF, 1)
    marks = jnp.where(c == 0, turned, gathered)
    share = jnp.exp(marks - jnp.max(marks, axis=0, keepdims=True))
    share_of = share * jnp.where(c == 0, gathered, turned)
    result = jnp.sum(share_of, axis=0, keepdims=True) / jnp.sum(share, axis=0, keepdims=True)
    out_ref[...] = result[:, :HALF].astype(BF16)
    pltpu.make_async_copy(send, send, send_sem).wait()


def shards(q_nope, q_rope, w_key_up, w_value_up, latent_cache, page_scale, block_table, lengths):
    hbm = pl.BlockSpec(memory_space=pl.ANY)
    dma = pltpu.SemaphoreType.DMA
    return pl.pallas_call(
        kernel,
        out_shape=pltpu.VMEM((1, HALF), BF16),
        in_specs=[hbm] * 8,
        out_specs=pl.BlockSpec(memory_space=pltpu.VMEM),
        scratch_shapes=[
            pltpu.VMEM((BATCH, HEADS, NOPE), BF16),
            pltpu.VMEM((BATCH, HEADS, ROPE), BF16),
            pltpu.VMEM((HEADS, NOPE, LAT), BF16),
            pltpu.VMEM((HEADS, LAT, VDIM), BF16),
            pltpu.VMEM((PAGES, PAGE, LAT + ROPE), BF16),
            pltpu.SMEM((PAGES,), F32),
            pltpu.VMEM((BATCH, BLOCKS), jnp.int32),
            pltpu.SMEM((BATCH,), jnp.int32),
            pltpu.VMEM((ROWS, NOPE), F32),
            pltpu.VMEM((ROWS, ROPE), F32),
            pltpu.VMEM((ROWS, LAT), F32),
            pltpu.VMEM((CHUNKS // SIDE, TILES, SPAN, LANES), F32),
            pltpu.VMEM((PAGES // 16, 8, LANES), F32),
            pltpu.VMEM((2 * (LAT + ROPE), LANES), BF16),
            pltpu.VMEM((2 * ROWS, 1, VDIM), F32),
            pltpu.VMEM((SOURCES + 1, 1, VDIM), F32),
            dma((6,)),
            dma((PIECES,)),
            dma((CHUNKS,)),
            dma,
            dma,
        ],
        compiler_params=pltpu.CompilerParams(collective_id=0, has_side_effects=True),
        name="latent_decode",
    )(q_nope, q_rope, w_key_up, w_value_up, latent_cache, page_scale, block_table, lengths)


def solution(mesh):
    split = Mesh(
        mesh.devices.reshape(8, 8, 2, mesh.shape["head"]), ("seq_0", "seq_1", "seq_2", "head")
    )
    return jax.shard_map(
        shards,
        mesh=split,
        in_specs=(
            P(None, "head", None),
            P(None, "head", None),
            P("head", None, None),
            P("head", None, None),
            P(SEQ, None, None),
            P(SEQ),
            P(None, SEQ),
            P(),
        ),
        out_specs=P("head", SEQ),
        check_vma=False,
    )
```

```python
import jax
import jax.numpy as jnp
from jax import lax
from jax.experimental import pallas as pl
from jax.experimental.pallas import tpu as pltpu
from jax.sharding import Mesh
from jax.sharding import PartitionSpec as P

SEQ = ("seq_0", "seq_1", "seq_2")
F32 = jnp.float32
BF16 = jnp.bfloat16

BATCH = 4
HEADS = 16
ROWS = BATCH * HEADS
LAT = 512
ROPE = 64
NOPE = 128
VDIM = 128
HALF = VDIM // 2
PAGE = 64
PAGES = 64
BLOCKS = 16
CHUNK = 8
CHUNKS = PAGES // CHUNK
SPAN = CHUNK * PAGE
PIECES = 4
PIECE = HEADS // PIECES
LANES = 128
SIDE = 4
PARTS = 2
TILES = 2
NX = 4
EARLY = 2
LATE = 8
UNROLL = 8
SOURCES = 128
FLOOR = -1e30


def place(rhs, first, depth, block):
    empty = jnp.zeros((depth, ROWS), BF16)
    rhs[pl.ds(first, depth), :] = jnp.concatenate([block, empty], axis=1)
    rhs[pl.ds(first + depth, depth), :] = jnp.concatenate([empty, block], axis=1)


def kernel(
    qn_hbm, qr_hbm, wk_hbm, wv_hbm, cache_hbm, ps_hbm, bt_hbm, len_hbm, out_ref,
    qn, qr, wk, wv, cache, ps, bt, ln, qs, qrs, ql, s_buf, vc, rhs, send, recv,
    in_sem, wk_sem, cache_sem, send_sem, recv_sem,
):
    z = lax.axis_index("seq_0")
    y = lax.axis_index("seq_1")
    c = lax.axis_index("seq_2")
    x = lax.axis_index("head")

    small = [
        pltpu.make_async_copy(src, dst, in_sem.at[k])
        for k, (src, dst) in enumerate(
            [(qn_hbm, qn), (qr_hbm, qr), (bt_hbm, bt), (len_hbm, ln), (ps_hbm, ps), (wv_hbm, wv)]
        )
    ]
    keys = [
        pltpu.make_async_copy(
            wk_hbm.at[pl.ds(k * PIECE, PIECE)], wk.at[pl.ds(k * PIECE, PIECE)], wk_sem.at[k]
        )
        for k in range(PIECES)
    ]
    pages = [
        pltpu.make_async_copy(
            cache_hbm.at[pl.ds(k * CHUNK, CHUNK)], cache.at[pl.ds(k * CHUNK, CHUNK)], cache_sem.at[k]
        )
        for k in range(CHUNKS)
    ]
    for copy in small[:5] + keys:
        copy.start()

    me = (z * 8 + y) * 2 + c
    plane = lax.div(z, 2)
    alone = plane == x
    other = me + 1 - 2 * c
    barrier = pltpu.get_barrier_semaphore()

    def greet(k):
        pl.semaphore_signal(
            barrier, inc=1, device_id=k * NX + plane, device_id_type=pl.DeviceIdType.LOGICAL
        )

    greet(jnp.where(alone, other, me))

    def greet_all(first, last):
        @pl.loop(first, last)
        def _(i):
            for j in range(1, UNROLL + 1):
                greet(lax.rem(me + i * UNROLL + j, SOURCES))

    greet_all(0, EARLY)
    for copy in pages[:SIDE]:
        copy.start()
    greet_all(EARLY, LATE)
    for copy in pages[SIDE:]:
        copy.start()
    greet_all(LATE, SOURCES // UNROLL - 1)
    for j in range(1, UNROLL):
        greet(lax.rem(me + SOURCES - UNROLL + j, SOURCES))

    for copy in small[:5] + keys:
        copy.wait()
    for b in range(BATCH):
        qs[pl.ds(b, HEADS, stride=BATCH), :] = qn[b].astype(F32)
        qrs[pl.ds(b, HEADS, stride=BATCH), :] = qr[b].astype(F32)

    request = lax.rem(lax.broadcasted_iota(jnp.int32, (PAGES, ROWS), 1), BATCH)
    page_id = lax.broadcasted_iota(jnp.int32, (PAGES, BLOCKS), 0)
    block = lax.broadcasted_iota(jnp.int32, (PAGES, BLOCKS), 1)
    valid = jnp.zeros((PAGES, ROWS), F32)
    for b in range(BATCH):
        left = jnp.clip(ln[b] - (me * BLOCKS + block) * PAGE, 0, PAGE).astype(F32)
        owned = jnp.where(jnp.broadcast_to(bt[b : b + 1, :], (PAGES, BLOCKS)) == page_id, left, 0.0)
        valid = jnp.where(request == b, jnp.sum(owned, axis=1, keepdims=True), valid)
    for g in range(PAGES // 16):
        vc[g] = jnp.concatenate([valid[16 * g : 16 * g + 8], valid[16 * g + 8 : 16 * g + 16]], axis=1)
    place(rhs, 2 * LAT, ROPE, qrs[pl.ds(0, ROWS), :].T.astype(BF16))

    for h in range(HEADS):
        lhs = qs[pl.ds(16 * (h // 4), 16), :].astype(BF16)
        part = jnp.dot(lhs, wk[h], preferred_element_type=F32)
        at = 4 * (h % 4)
        ql[pl.ds(4 * h, 4), :] = part[at : at + 4]
    place(rhs, 0, LAT, ql[...].T.astype(BF16))

    small[5].start()
    row_id = lax.broadcasted_iota(jnp.int32, (PAGE, LANES), 0).astype(F32)
    even = lax.broadcasted_iota(jnp.int32, (1, LANES), 1) < ROWS

    def scale_of(s, tile, page):
        p = (s * SIDE + 2 * tile) * CHUNK + page
        return jnp.where(even, ps[p], ps[p + CHUNK])

    def products(s):
        for i in range(SIDE):
            pages[s * SIDE + i].wait()
        raw = []
        for tile in range(TILES):
            here = [pl.ds((s * SIDE + 2 * tile + i) * CHUNK, CHUNK) for i in range(2)]
            lhs = [cache[at, :, :LAT].reshape(SPAN, LAT) for at in here]
            lhs = lhs + [cache[at, :, LAT:].reshape(SPAN, ROPE) for at in here]
            lhs = jnp.concatenate(lhs, axis=1)
            halves = [lhs[: SPAN // 2], lhs[SPAN // 2 :]]
            raw.append(
                jnp.concatenate([jnp.dot(m, rhs[...], preferred_element_type=F32) for m in halves], axis=0)
            )
        return raw

    def scores(s, raw):
        peak = jnp.full((PAGE, LANES), FLOOR, F32)
        for page in range(CHUNK):
            for tile in range(TILES):
                scale = scale_of(s, tile, page) * (NOPE + ROPE) ** (-0.5)
                scaled = raw[tile][page * PAGE : (page + 1) * PAGE] * scale
                score = jnp.where(row_id < vc[s * TILES + tile, pl.ds(page, 1), :], scaled, FLOOR)
                s_buf[s, tile, pl.ds(page * PAGE, PAGE), :] = score
                peak = jnp.maximum(peak, score)
        peak = jnp.max(peak, axis=0, keepdims=True)
        return jnp.maximum(peak, pltpu.roll(peak, ROWS, 1))

    def weighted(s, floor):
        total = jnp.zeros((PAGE, LANES), F32)
        latent = [jnp.zeros((ROWS, LAT // PARTS), F32) for _ in range(PARTS)]
        for tile in range(TILES):
            pieces = []
            for page in range(CHUNK):
                weight = jnp.exp(s_buf[s, tile, pl.ds(page * PAGE, PAGE), :] - floor)
                total = total + weight
                pieces.append(weight * scale_of(s, tile, page))
            prob = jnp.concatenate(pieces, axis=0).T.astype(BF16)
            for i in range(2):
                k = s * SIDE + 2 * tile + i
                for part in range(PARTS):
                    columns = pl.ds(part * (LAT // PARTS), LAT // PARTS)
                    lat_rows = cache[pl.ds(k * CHUNK, CHUNK), :, columns].reshape(SPAN, LAT // PARTS)
                    latent[part] = latent[part] + jnp.dot(
                        prob[i * ROWS : (i + 1) * ROWS], lat_rows, preferred_element_type=F32
                    )
        total = jnp.sum(total, axis=0, keepdims=True)
        return total + pltpu.roll(total, ROWS, 1), jnp.concatenate(latent, axis=1)

    raw = [products(s) for s in range(CHUNKS // SIDE)]
    former = jnp.maximum(scores(0, raw[0]), -1e29)
    floor = jnp.maximum(scores(1, raw[1]), former)
    total, latent = weighted(0, former)
    total_two, latent_two = weighted(1, floor)
    correction = jnp.exp(former - floor)
    denominator = total * correction + total_two

    some = denominator > 0.0
    safe = jnp.where(some, denominator, 1.0)
    level = jnp.where(some, floor + jnp.log(safe), FLOOR)
    sub = lax.broadcasted_iota(jnp.int32, (8, LANES), 0)
    inverse = 1.0 / safe
    columns = jnp.where(sub == 0, level, jnp.where(sub == 1, inverse, correction * inverse)).T
    level = jnp.broadcast_to(columns[:ROWS, 0:1], (ROWS, VDIM))
    latent = (latent * columns[:ROWS, 2:3] + latent_two * columns[:ROWS, 1:2]).astype(BF16)

    small[5].wait()
    pl.semaphore_wait(barrier, SOURCES)
    sub = lax.broadcasted_iota(jnp.int32, (8, VDIM), 0)
    low = lax.broadcasted_iota(jnp.int32, (8, VDIM), 1) < HALF
    data_lane = (sub < BATCH) == low
    rows = send.reshape(2 * ROWS, VDIM)
    mine = lax.rem(me * NX + x, SOURCES)

    def post(t, slot, to):
        pltpu.make_async_remote_copy(
            src_ref=send.at[t],
            dst_ref=recv.at[slot],
            send_sem=send_sem,
            recv_sem=recv_sem,
            device_id=to,
            device_id_type=pl.DeviceIdType.LOGICAL,
        ).start()

    def project(h):
        part = jnp.dot(latent[16 * (h // 4) : 16 * (h // 4) + 16], wv[h], preferred_element_type=F32)
        at = 4 * (h % 4)
        part = part[at : at + 4]
        mark = level[4 * h : 4 * h + 4]
        rows[pl.ds(8 * h, 8), :] = jnp.where(
            data_lane, jnp.concatenate([part, part], axis=0), jnp.concatenate([mark, mark], axis=0)
        )

    project(0)
    for t in (4, 5, 6, 7, 0, 1, 2, 3):
        is_self = jnp.logical_and(alone, mine == t)
        post(t, jnp.where(is_self, SOURCES, me), SOURCES * x + jnp.where(is_self, t ^ NX, t))
    for h in range(1, HEADS):
        project(h)

    @pl.loop(1, SOURCES // UNROLL)
    def _(i):
        for j in range(UNROLL):
            t = i * UNROLL + j
            is_self = jnp.logical_and(alone, mine == t)
            turned = SOURCES * x + t + jnp.where(is_self, NX * (1 - 2 * c), 0)
            post(t, jnp.where(is_self, SOURCES, me), turned)

    @pl.when(alone)
    def _():
        recv[me] = send[mine]

    pltpu.make_async_copy(recv.at[pl.ds(0, SOURCES)], recv.at[pl.ds(0, SOURCES)], recv_sem).wait()

    gathered = recv.reshape(SOURCES + 1, VDIM)[pl.ds(0, SOURCES), :]
    turned = pltpu.roll(gathered, HALF, 1)
    marks = jnp.where(c == 0, turned, gathered)
    share = jnp.exp(marks - jnp.max(marks, axis=0, keepdims=True))
    share_of = share * jnp.where(c == 0, gathered, turned)
    result = jnp.sum(share_of, axis=0, keepdims=True) / jnp.sum(share, axis=0, keepdims=True)
    out_ref[...] = result[:, :HALF].astype(BF16)
    pltpu.make_async_copy(send, send, send_sem).wait()


def shards(q_nope, q_rope, w_key_up, w_value_up, latent_cache, page_scale, block_table, lengths):
    hbm = pl.BlockSpec(memory_space=pl.ANY)
    dma = pltpu.SemaphoreType.DMA
    return pl.pallas_call(
        kernel,
        out_shape=pltpu.VMEM((1, HALF), BF16),
        in_specs=[hbm] * 8,
        out_specs=pl.BlockSpec(memory_space=pltpu.VMEM),
        scratch_shapes=[
            pltpu.VMEM((BATCH, HEADS, NOPE), BF16),
            pltpu.VMEM((BATCH, HEADS, ROPE), BF16),
            pltpu.VMEM((HEADS, NOPE, LAT), BF16),
            pltpu.VMEM((HEADS, LAT, VDIM), BF16),
            pltpu.VMEM((PAGES, PAGE, LAT + ROPE), BF16),
            pltpu.SMEM((PAGES,), F32),
            pltpu.VMEM((BATCH, BLOCKS), jnp.int32),
            pltpu.SMEM((BATCH,), jnp.int32),
            pltpu.VMEM((ROWS + 8, NOPE), F32),
            pltpu.VMEM((ROWS + 8, ROPE), F32),
            pltpu.VMEM((ROWS, LAT), F32),
            pltpu.VMEM((CHUNKS // SIDE, TILES, SPAN, LANES), F32),
            pltpu.VMEM((PAGES // 16, 8, LANES), F32),
            pltpu.VMEM((2 * (LAT + ROPE), LANES), BF16),
            pltpu.VMEM((2 * ROWS, 1, VDIM), F32),
            pltpu.VMEM((SOURCES + 1, 1, VDIM), F32),
            dma((6,)),
            dma((PIECES,)),
            dma((CHUNKS,)),
            dma,
            dma,
        ],
        compiler_params=pltpu.CompilerParams(collective_id=0, has_side_effects=True),
        name="latent_decode",
    )(q_nope, q_rope, w_key_up, w_value_up, latent_cache, page_scale, block_table, lengths)


def solution(mesh):
    split = Mesh(
        mesh.devices.reshape(8, 8, 2, mesh.shape["head"]), ("seq_0", "seq_1", "seq_2", "head")
    )
    return jax.shard_map(
        shards,
        mesh=split,
        in_specs=(
            P(None, "head", None),
            P(None, "head", None),
            P("head", None, None),
            P("head", None, None),
            P(SEQ, None, None),
            P(SEQ),
            P(None, SEQ),
            P(),
        ),
        out_specs=P("head", SEQ),
        check_vma=False,
    )
```
